16 devices in a mesh: rep: 4 (over y, z, core), pp: 4 (over x).
Axes of the slice: x: 4, y: 2, z: 1, core: 2. Of those that a mesh axis runs over, the one named last changes fastest.
The devices are a block of a 4x4x8 slice.
Arguments:
- x: bfloat16 [32, 512, 512], P('rep'), parts along dimension 0
- dy: bfloat16 [32, 512, 512], P('rep'), parts along dimension 0
- w_gate: bfloat16 [4, 512, 1664], P('pp')
- w_up: bfloat16 [4, 512, 1664], P('pp')
- w_down: bfloat16 [4, 1664, 512], P('pp')
Outputs:
- output 1: bfloat16 [16, 512, 1664], P(('rep', 'pp')), parts along dimension 0
- output 2: bfloat16 [16, 512, 1664], P(('rep', 'pp')), parts along dimension 0
- output 3: bfloat16 [16, 1664, 512], P(('rep', 'pp')), parts along dimension 0
There are 4 independent parts. The reference program is written for one: setup_inputs(seed, part) draws one part's arguments, and reference() takes and returns one part's arrays. A program takes and returns all parts, laid end to end along the dimension named above; an argument that names none is the same for every part.
All inputs are finite; a program needn't handle non-finite values.
Results may differ from the reference program's by a relative error of at most 0.018.
Values are sent between devices in bfloat16 or wider.
A program may use at most 768 MiB of HBM per device.

```python
import jax
import jax.numpy as jnp
from jax import lax

MICRO = 8
TOKENS = 512
D = 512
FF = 1664
LAYERS = 4
NAMES = ("w_gate", "w_up", "w_down")
SHAPES = {"w_gate": (LAYERS, D, FF), "w_up": (LAYERS, D, FF), "w_down": (LAYERS, FF, D)}


def bump(key, n, height):
    away = (jnp.arange(n, dtype=jnp.int32) - jax.random.randint(key, (), 0, n, jnp.int32)) % n
    return jnp.where(away < n // 8, height, 1.0)


def together(key, own, strength):
    shared = jax.random.normal(key, own.shape[1:], jnp.float32)
    return (own + strength * shared) * lax.rsqrt(1 + strength * strength)


def setup_inputs(seed: int = 0, part: int = 0) -> dict:
    kx, kdy, ka, kb, kz, kf, kh, kl, *kw = jax.random.split(jax.random.key(seed), 8 + len(NAMES))
    kx, kdy, ka, kb = (jax.random.fold_in(k, part) for k in (kx, kdy, ka, kb))
    shape = (MICRO, TOKENS, D)
    much_x, much_dy = jax.random.uniform(kz, (2,), jnp.float32, 0.0, 1.0)
    layers = 2.0 ** jax.random.uniform(kl, (LAYERS, 1, 1), jnp.float32, -1.0, 1.0)
    x = together(ka, jax.random.normal(kx, shape, jnp.float32), much_x) * bump(kf, D, 4.0)
    dy = together(kb, jax.random.normal(kdy, shape, jnp.float32), much_dy)
    drawn = {"x": x.astype(jnp.bfloat16), "dy": (dy * (MICRO * TOKENS) ** -0.5).astype(jnp.bfloat16)}
    for key, name in zip(kw, NAMES, strict=True):
        w = jax.random.normal(key, SHAPES[name], jnp.float32) * SHAPES[name][1] ** -0.5
        drawn[name] = (w * {"w_gate": 1.0, "w_up": bump(kh, FF, 4.0), "w_down": layers}[name]).astype(jnp.bfloat16)
    return drawn


def matmul(a, w):
    return jnp.dot(a, w, preferred_element_type=jnp.float32).astype(jnp.bfloat16)


def normed(h):
    wide = h.astype(jnp.float32)
    scale = lax.rsqrt(jnp.mean(wide**2, -1, keepdims=True) + 1e-6)
    return (wide * scale).astype(jnp.bfloat16)


def layer(h, w):
    a = normed(h)
    gate = jnp.dot(a, w["w_gate"], preferred_element_type=jnp.float32)
    up = jnp.dot(a, w["w_up"], preferred_element_type=jnp.float32)
    return h + matmul((jax.nn.silu(gate) * up).astype(jnp.bfloat16), w["w_down"])


def stack(weights, h):
    return lax.scan(lambda h, w: (layer(h, w), None), h, weights)[0]


def reference(x, dy, w_gate, w_up, w_down):
    weights = dict(zip(NAMES, (w_gate, w_up, w_down), strict=True))

    def take(so_far, one):
        h, by_y = one
        _, back = jax.vjp(lambda w: stack(w, h), weights)
        return jax.tree.map(lambda total, term: total + term.astype(jnp.float32), so_far, back(by_y)[0]), None

    none_yet = {name: jnp.zeros(w.shape, jnp.float32) for name, w in weights.items()}
    by_weights, _ = lax.scan(take, none_yet, (x, dy))
    return tuple(by_weights[name].astype(jnp.bfloat16) for name in NAMES)
```

```python
import functools

import jax
import jax.numpy as jnp
from jax import lax
from jax.experimental import pallas as pl
from jax.experimental.pallas import tpu as pltpu
from jax.sharding import PartitionSpec as P

CHUNK = 128
BLOCK = 256
HALF = BLOCK // 2
OFF = 5
EPS = 1e-6
F32, BF16 = jnp.float32, jnp.bfloat16
MESH = pl.DeviceIdType.MESH


def dot(a, b):
    return jnp.dot(a, b, preferred_element_type=F32)


def sigmoid(x):
    return 0.5 * jnp.tanh(0.5 * x) + 0.5


def kernel(
    stages, per, chunks,
    x_ref, dy_ref, wg_ref, wu_ref, wd_ref,
    og_ref, ou_ref, od_ref,
    kept, byin, out, wgu, wgut, wd, wdt, rhs, lhs, total, midc, dguc,
    fsend, frecv, bsend, brecv, wsem, osem,
):
    me = lax.axis_index("pp")
    behind = stages - 1 - me
    first, last = me == 0, behind == 0
    right, left = lax.rem(me + 1, stages), lax.rem(me + stages - 1, stages)
    d, ff = wg_ref.shape
    nb = ff // HALF
    nd = pl.cdiv(ff, BLOCK)
    quarter = (nb + nd) // per

    loads = [pltpu.make_async_copy(wd_ref, wd, wsem.at[0])]
    for j in range(nb):
        cols = pl.ds(j * HALF, HALF)
        loads.append(pltpu.make_async_copy(wg_ref.at[:, cols], wgu.at[j, :, pl.ds(0, HALF)], wsem.at[1 + 2 * j]))
        loads.append(pltpu.make_async_copy(wu_ref.at[:, cols], wgu.at[j, :, pl.ds(HALF, HALF)], wsem.at[2 + 2 * j]))
    for load in loads:
        load.start()

    def x_load(k):
        return pltpu.make_async_copy(x_ref.at[k], kept.at[k], frecv.at[k])

    def dy_load(k):
        return pltpu.make_async_copy(dy_ref.at[k], byin.at[k], brecv.at[k])

    @pl.when(first)
    def _():
        def go(k, c):
            x_load(k).start()
            return c

        lax.fori_loop(0, chunks, go, 0)

    @pl.when(last)
    def _():
        def go(k, c):
            dy_load(k).start()
            return c

        lax.fori_loop(0, chunks, go, 0)

    barrier = pltpu.get_barrier_semaphore()
    for side in (left, right):
        pl.semaphore_signal(barrier, inc=1, device_id={"pp": side}, device_id_type=MESH)

    total[...] = jnp.zeros_like(total)
    rhs[:, nb + nd - 1] = jnp.zeros_like(rhs[:, nb + nd - 1])
    wdt[nd - 1] = jnp.zeros_like(wdt[nd - 1])
    for load in loads:
        load.wait()
    pl.semaphore_wait(barrier, 2)

    def f_copy(k):
        return pltpu.make_async_remote_copy(
            src_ref=out.at[k], dst_ref=kept.at[k], send_sem=fsend.at[k], recv_sem=frecv.at[k],
            device_id={"pp": right}, device_id_type=MESH,
        )

    def b_copy(k):
        return pltpu.make_async_remote_copy(
            src_ref=out.at[k], dst_ref=byin.at[k], send_sem=bsend.at[k], recv_sem=brecv.at[k],
            device_id={"pp": left}, device_id_type=MESH,
        )

    def normed(h):
        wide = h.astype(F32)
        scale = lax.rsqrt(jnp.mean(wide * wide, -1, keepdims=True) + EPS)
        return wide, scale, (wide * scale).astype(BF16)

    def forward(k):
        x_load(k).wait()
        wide, _, a = normed(kept[k])
        for j in range(nb):
            gu = dot(a, wgu[j])
            g, u = gu[:, :HALF], gu[:, HALF:]
            midc[:, j * HALF : (j + 1) * HALF] = (g * sigmoid(g) * u).astype(BF16)
        y = dot(midc[...], wd[...]).astype(BF16)
        out[k] = (wide + y.astype(F32)).astype(BF16)
        f_copy(k).start()

    def backward(k):
        slot = lax.rem(lax.div(k, per), 2)
        rows = pl.ds(pl.multiple_of(lax.rem(k, per) * CHUNK, CHUNK), CHUNK)

        @pl.when(last)
        def _():
            x_load(k).wait()

        dy_load(k).wait()

        @pl.when(jnp.logical_not(last))
        def _():
            f_copy(k).wait_send()

        by = byin[k]
        wide, scale, a = normed(kept[k])
        lhs[slot, 0, :, rows] = a.astype(F32).T.astype(BF16)
        lhs[slot, 1, :, rows] = by.astype(F32).T.astype(BF16)
        for jj in range(nd):
            dmid2 = dot(by, wdt[jj]).astype(BF16).astype(F32)
            for part in range(2):
                j = 2 * jj + part
                if j >= nb:
                    break
                dmid = dmid2[:, part * HALF : (part + 1) * HALF]
                gu = dot(a, wgu[j])
                g, u = gu[:, :HALF], gu[:, HALF:]
                s = sigmoid(g)
                silu = g * s
                dup = (dmid * silu).astype(BF16)
                dgate = (dmid * u * (s + silu * (1.0 - s))).astype(BF16)
                rhs[slot, nb + jj, rows, part * HALF : (part + 1) * HALF] = (silu * u).astype(BF16)
                rhs[slot, j, rows, :HALF] = dgate
                rhs[slot, j, rows, HALF:] = dup
                dguc[:, j * BLOCK : j * BLOCK + HALF] = dgate
                dguc[:, j * BLOCK + HALF : (j + 1) * BLOCK] = dup

        @pl.when(jnp.logical_not(first))
        def _():
            wide, scale, _ = normed(kept[k])
            da = dot(dguc[...], wgut[...]).astype(BF16).astype(F32)
            lean = jnp.mean(da * wide, -1, keepdims=True) * scale * scale * scale
            dh = (da * scale - wide * lean).astype(BF16)
            out[k] = (byin[k].astype(F32) + dh.astype(F32)).astype(BF16)
            b_copy(k).start()

    def products(k):
        slot = lax.rem(lax.div(k, per), 2)
        start = lax.rem(k, per) * quarter
        for i in range(quarter):
            q = start + i
            which = jnp.where(q >= nb, 1, 0)
            term = dot(lhs[slot, which], rhs[slot, q]).astype(BF16)
            total[q] += term.astype(F32)

    def transposed():
        for j in range(nb):
            wgut[j * BLOCK : (j + 1) * BLOCK, :] = wgu[j].astype(F32).T.astype(BF16)
        for jj in range(nd):
            lo, hi = jj * BLOCK, min(ff, (jj + 1) * BLOCK)
            wdt[jj, :, : hi - lo] = wd[lo:hi, :].astype(F32).T.astype(BF16)

    def step(i, carry):
        f, b = i, i - OFF * behind
        w = b - per

        @pl.when((f < chunks) & jnp.logical_not(last))
        def _():
            forward(f)

        @pl.when(i == jnp.where(first, 3, 0))
        def _():
            transposed()

        @pl.when((b >= 0) & (b < chunks))
        def _():
            backward(b)

        @pl.when((w >= 0) & (w < chunks))
        def _():
            products(w)

        return carry

    lax.fori_loop(0, chunks + OFF * (stages - 1) + per, step, 0)

    stores = []
    for jj in range(nd):
        lo, hi = jj * BLOCK, min(ff, (jj + 1) * BLOCK)
        wd[lo:hi, :] = total[nb + jj].T[: hi - lo].astype(BF16)
    stores.append(pltpu.make_async_copy(wd, od_ref, osem.at[0]))
    stores[-1].start()
    for j in range(nb):
        cols = pl.ds(j * HALF, HALF)
        rhs[0, j] = total[j].astype(BF16)
        stores.append(pltpu.make_async_copy(rhs.at[0, j, :, pl.ds(0, HALF)], og_ref.at[:, cols], osem.at[1 + 2 * j]))
        stores[-1].start()
        stores.append(pltpu.make_async_copy(rhs.at[0, j, :, pl.ds(HALF, HALF)], ou_ref.at[:, cols], osem.at[2 + 2 * j]))
        stores[-1].start()
    for store in stores:
        store.wait()

    @pl.when(jnp.logical_not(first))
    def _():
        def sent(k, c):
            b_copy(k).wait_send()
            return c

        lax.fori_loop(0, chunks, sent, 0)


def solution(mesh):
    stages = mesh.shape["pp"]

    def step(x, dy, w_gate, w_up, w_down):
        micro, tokens, d = x.shape
        ff = w_gate.shape[-1]
        per = tokens // CHUNK
        chunks = micro * per
        nb, nd = ff // HALF, pl.cdiv(ff, BLOCK)
        flat = (chunks, CHUNK, d)
        grads = pl.pallas_call(
            functools.partial(kernel, stages, per, chunks),
            out_shape=[
                jax.ShapeDtypeStruct((d, ff), BF16),
                jax.ShapeDtypeStruct((d, ff), BF16),
                jax.ShapeDtypeStruct((ff, d), BF16),
            ],
            in_specs=[pl.BlockSpec(memory_space=pl.ANY)] * 5,
            out_specs=[pl.BlockSpec(memory_space=pl.ANY)] * 3,
            scratch_shapes=[
                pltpu.VMEM(flat, BF16),
                pltpu.VMEM(flat, BF16),
                pltpu.VMEM(flat, BF16),
                pltpu.VMEM((nb, d, BLOCK), BF16),
                pltpu.VMEM((nb * BLOCK, d), BF16),
                pltpu.VMEM((ff, d), BF16),
                pltpu.VMEM((nd, d, BLOCK), BF16),
                pltpu.VMEM((2, nb + nd, tokens, BLOCK), BF16),
                pltpu.VMEM((2, 2, d, tokens), BF16),
                pltpu.VMEM((nb + nd, d, BLOCK), F32),
                pltpu.VMEM((CHUNK, ff), BF16),
                pltpu.VMEM((CHUNK, nb * BLOCK), BF16),
                pltpu.SemaphoreType.DMA((chunks,)),
                pltpu.SemaphoreType.DMA((chunks,)),
                pltpu.SemaphoreType.DMA((chunks,)),
                pltpu.SemaphoreType.DMA((chunks,)),
                pltpu.SemaphoreType.DMA((1 + 2 * nb,)),
                pltpu.SemaphoreType.DMA((1 + 2 * nb,)),
            ],
            compiler_params=pltpu.CompilerParams(
                collective_id=0, has_side_effects=True, vmem_limit_bytes=67_000_000
            ),
        )(x.reshape(flat), dy.reshape(flat), w_gate[0], w_up[0], w_down[0])
        return tuple(g[None] for g in grads)

    return jax.shard_map(
        step,
        mesh=mesh,
        in_specs=(P("rep", None, None),) * 2 + (P("pp", None, None),) * 3,
        out_specs=(P(("rep", "pp"), None, None),) * 3,
        check_vma=False,
    )
```

```python
import functools

import jax
import jax.numpy as jnp
from jax import lax
from jax.experimental import pallas as pl
from jax.experimental.pallas import tpu as pltpu
from jax.sharding import PartitionSpec as P

CHUNK = 128
BLOCK = 256
HALF = BLOCK // 2
OFF = 5
AHEAD = 5
OUT = 4
EPS = 1e-6
F32, BF16 = jnp.float32, jnp.bfloat16
MESH = pl.DeviceIdType.MESH


def dot(a, b):
    return jnp.dot(a, b, preferred_element_type=F32)


def sigmoid(x):
    return 0.5 * jnp.tanh(0.5 * x) + 0.5


def kernel(
    stages, per, chunks,
    x_ref, dy_ref, wg_ref, wu_ref, wd_ref,
    og_ref, ou_ref, od_ref,
    kept, byin, fout, bout, wgu, wgut, wd, wdt, rhs, lhs, total, mids, slopes, dguc,
    fsend, frecv, bsend, brecv, wsem, osem,
):
    me = lax.axis_index("pp")
    behind = stages - 1 - me
    first, last = me == 0, behind == 0
    right, left = lax.rem(me + 1, stages), lax.rem(me + stages - 1, stages)
    d, ff = wg_ref.shape
    nb = ff // HALF
    nd = pl.cdiv(ff, BLOCK)
    quarter = (nb + nd) // per

    loads = [pltpu.make_async_copy(wd_ref, wd, wsem.at[0])]
    for j in range(nb):
        cols = pl.ds(j * HALF, HALF)
        loads.append(pltpu.make_async_copy(wg_ref.at[:, cols], wgu.at[j, :, pl.ds(0, HALF)], wsem.at[1 + 2 * j]))
        loads.append(pltpu.make_async_copy(wu_ref.at[:, cols], wgu.at[j, :, pl.ds(HALF, HALF)], wsem.at[2 + 2 * j]))
    for load in loads:
        load.start()

    reach = OFF * (stages - 1)
    n_kept, n_by, n_mid = kept.shape[0], byin.shape[0], mids.shape[0]
    assert n_kept > reach and n_by > reach and n_mid > OFF * (stages - 2)

    def x_load(k):
        return pltpu.make_async_copy(x_ref.at[k], kept.at[lax.rem(k, n_kept)], frecv.at[k])

    def dy_load(k):
        return pltpu.make_async_copy(dy_ref.at[k], byin.at[lax.rem(k, n_by)], brecv.at[k])

    @pl.when(first)
    def _():
        def go(k, c):
            x_load(k).start()
            return c

        lax.fori_loop(0, min(chunks, n_kept), go, 0)

    @pl.when(last)
    def _():
        def go(k, c):
            dy_load(k).start()
            return c

        lax.fori_loop(0, min(chunks, n_by), go, 0)

    barrier = pltpu.get_barrier_semaphore()
    for side in (left, right):
        pl.semaphore_signal(barrier, inc=1, device_id={"pp": side}, device_id_type=MESH)

    total[...] = jnp.zeros_like(total)
    rhs[:, nb + nd - 1] = jnp.zeros_like(rhs[:, nb + nd - 1])
    wdt[nd - 1] = jnp.zeros_like(wdt[nd - 1])
    for load in loads:
        load.wait()
    pl.semaphore_wait(barrier, 2)

    def f_copy(k):
        return pltpu.make_async_remote_copy(
            src_ref=fout.at[lax.rem(k, OUT)], dst_ref=kept.at[lax.rem(k, n_kept)], send_sem=fsend.at[k], recv_sem=frecv.at[k],
            device_id={"pp": right}, device_id_type=MESH,
        )

    def b_copy(k):
        return pltpu.make_async_remote_copy(
            src_ref=bout.at[lax.rem(k, OUT)], dst_ref=byin.at[lax.rem(k, n_by)], send_sem=bsend.at[k], recv_sem=brecv.at[k],
            device_id={"pp": left}, device_id_type=MESH,
        )

    def normed(h):
        wide = h.astype(F32)
        scale = lax.rsqrt(jnp.mean(wide * wide, -1, keepdims=True) + EPS)
        return wide, scale, (wide * scale).astype(BF16)

    def forward(k):
        x_load(k).wait()
        slot = lax.rem(k, n_mid)
        wide, _, a = normed(kept[lax.rem(k, n_kept)])
        for j in range(nb):
            gu = dot(a, wgu[j])
            g, u = gu[:, :HALF], gu[:, HALF:]
            s = sigmoid(g)
            silu = g * s
            mids[slot, :, j * HALF : (j + 1) * HALF] = (silu * u).astype(BF16)
            slopes[slot, j, :, :HALF] = u * (s + silu * (1.0 - s))
            slopes[slot, j, :, HALF:] = silu
        y = dot(mids[slot], wd[...]).astype(BF16)

        @pl.when(k >= OUT)
        def _():
            f_copy(k - OUT).wait_send()

        fout[lax.rem(k, OUT)] = (wide + y.astype(F32)).astype(BF16)
        f_copy(k).start()

    def backward(k):
        slot = lax.rem(lax.div(k, per), 2)
        mine = lax.rem(k, n_mid)
        here = lax.rem(k, n_kept)
        rows = pl.ds(pl.multiple_of(lax.rem(k, per) * CHUNK, CHUNK), CHUNK)

        @pl.when(last)
        def _():
            x_load(k).wait()

        dy_load(k).wait()

        def share(j, dmid, slope, silu, mid):
            jj, part = j // 2, j % 2
            dgate, dup = (dmid * slope).astype(BF16), (dmid * silu).astype(BF16)
            rhs[slot, nb + jj, rows, part * HALF : (part + 1) * HALF] = mid
            rhs[slot, j, rows, :HALF] = dgate
            rhs[slot, j, rows, HALF:] = dup
            dguc[:, j * BLOCK : j * BLOCK + HALF] = dgate
            dguc[:, j * BLOCK + HALF : (j + 1) * BLOCK] = dup

        def by_mid(by):
            for jj in range(nd):
                two = dot(by, wdt[jj]).astype(BF16).astype(F32)
                for part in range(min(2, nb - 2 * jj)):
                    yield 2 * jj + part, two[:, part * HALF : (part + 1) * HALF]

        def turned(a, by):
            lhs[slot, 0, :, rows] = a.astype(F32).T.astype(BF16)
            lhs[slot, 1, :, rows] = by.astype(F32).T.astype(BF16)

        @pl.when(first | last)
        def _():
            by = byin[lax.rem(k, n_by)]
            _, _, a = normed(kept[here])
            turned(a, by)
            for j, dmid in by_mid(by):
                gu = dot(a, wgu[j])
                g, u = gu[:, :HALF], gu[:, HALF:]
                s = sigmoid(g)
                silu = g * s
                share(j, dmid, u * (s + silu * (1.0 - s)), silu, (silu * u).astype(BF16))

        @pl.when(jnp.logical_not(first | last))
        def _():
            by = byin[lax.rem(k, n_by)]
            _, _, a = normed(kept[here])
            turned(a, by)
            for j, dmid in by_mid(by):
                share(j, dmid, slopes[mine, j, :, :HALF], slopes[mine, j, :, HALF:], mids[mine, :, j * HALF : (j + 1) * HALF])

        @pl.when(jnp.logical_not(first))
        def _():
            wide, scale, _ = normed(kept[here])
            da = dot(dguc[...], wgut[...]).astype(BF16).astype(F32)
            lean = jnp.mean(da * wide, -1, keepdims=True) * scale * scale * scale
            dh = (da * scale - wide * lean).astype(BF16)

            @pl.when(k >= OUT)
            def _():
                b_copy(k - OUT).wait_send()

            bout[lax.rem(k, OUT)] = (byin[lax.rem(k, n_by)].astype(F32) + dh.astype(F32)).astype(BF16)
            b_copy(k).start()

        @pl.when(first & (k + n_kept < chunks))
        def _():
            x_load(k + n_kept).start()

        @pl.when(last & (k + n_by < chunks))
        def _():
            dy_load(k + n_by).start()

    def products(k):
        slot = lax.rem(lax.div(k, per), 2)
        start = lax.rem(k, per) * quarter
        for i in range(quarter):
            q = start + i
            which = jnp.where(q >= nb, 1, 0)
            term = dot(lhs[slot, which], rhs[slot, q]).astype(BF16)
            total[q] += term.astype(F32)

    def transposed():
        for j in range(nb):
            wgut[j * BLOCK : (j + 1) * BLOCK, :] = wgu[j].astype(F32).T.astype(BF16)
        for jj in range(nd):
            lo, hi = jj * BLOCK, min(ff, (jj + 1) * BLOCK)
            wdt[jj, :, : hi - lo] = wd[lo:hi, :].astype(F32).T.astype(BF16)

    def step(i, carry):
        f, b = i, i - OFF * behind
        w = b - per

        @pl.when(i == jnp.where(first, 3, 0))
        def _():
            transposed()

        @pl.when((f < chunks) & jnp.logical_not(last))
        def _():
            forward(f)

        @pl.when((b >= 0) & (b < chunks))
        def _():
            backward(b)

        @pl.when((w >= 0) & (w < chunks))
        def _():
            products(w)

        return carry

    lax.fori_loop(0, chunks + OFF * (stages - 1) + per, step, 0)

    stores = []
    for jj in range(nd):
        lo, hi = jj * BLOCK, min(ff, (jj + 1) * BLOCK)
        wd[lo:hi, :] = total[nb + jj].T[: hi - lo].astype(BF16)
    stores.append(pltpu.make_async_copy(wd, od_ref, osem.at[0]))
    stores[-1].start()
    for j in range(nb):
        cols = pl.ds(j * HALF, HALF)
        rhs[0, j] = total[j].astype(BF16)
        stores.append(pltpu.make_async_copy(rhs.at[0, j, :, pl.ds(0, HALF)], og_ref.at[:, cols], osem.at[1 + 2 * j]))
        stores[-1].start()
        stores.append(pltpu.make_async_copy(rhs.at[0, j, :, pl.ds(HALF, HALF)], ou_ref.at[:, cols], osem.at[2 + 2 * j]))
        stores[-1].start()
    for store in stores:
        store.wait()

    def sent(copy):
        def one(k, c):
            copy(k).wait_send()
            return c

        lax.fori_loop(max(0, chunks - OUT), chunks, one, 0)

    @pl.when(jnp.logical_not(last))
    def _():
        sent(f_copy)

    @pl.when(jnp.logical_not(first))
    def _():
        sent(b_copy)


def solution(mesh):
    stages = mesh.shape["pp"]

    def step(x, dy, w_gate, w_up, w_down):
        micro, tokens, d = x.shape
        ff = w_gate.shape[-1]
        per = tokens // CHUNK
        chunks = micro * per
        nb, nd = ff // HALF, pl.cdiv(ff, BLOCK)
        flat = (chunks, CHUNK, d)
        reach, saved = OFF * (stages - 1), OFF * (stages - 2) + 1
        grads = pl.pallas_call(
            functools.partial(kernel, stages, per, chunks),
            out_shape=[
                jax.ShapeDtypeStruct((d, ff), BF16),
                jax.ShapeDtypeStruct((d, ff), BF16),
                jax.ShapeDtypeStruct((ff, d), BF16),
            ],
            in_specs=[pl.BlockSpec(memory_space=pl.ANY)] * 5,
            out_specs=[pl.BlockSpec(memory_space=pl.ANY)] * 3,
            scratch_shapes=[
                pltpu.VMEM((reach + AHEAD, CHUNK, d), BF16),
                pltpu.VMEM((reach + 1, CHUNK, d), BF16),
                pltpu.VMEM((OUT, CHUNK, d), BF16),
                pltpu.VMEM((OUT, CHUNK, d), BF16),
                pltpu.VMEM((nb, d, BLOCK), BF16),
                pltpu.VMEM((nb * BLOCK, d), BF16),
                pltpu.VMEM((ff, d), BF16),
                pltpu.VMEM((nd, d, BLOCK), BF16),
                pltpu.VMEM((2, nb + nd, tokens, BLOCK), BF16),
                pltpu.VMEM((2, 2, d, tokens), BF16),
                pltpu.VMEM((nb + nd, d, BLOCK), F32),
                pltpu.VMEM((saved, CHUNK, ff), BF16),
                pltpu.VMEM((saved, nb, CHUNK, BLOCK), F32),
                pltpu.VMEM((CHUNK, nb * BLOCK), BF16),
                pltpu.SemaphoreType.DMA((chunks,)),
                pltpu.SemaphoreType.DMA((chunks,)),
                pltpu.SemaphoreType.DMA((chunks,)),
                pltpu.SemaphoreType.DMA((chunks,)),
                pltpu.SemaphoreType.DMA((1 + 2 * nb,)),
                pltpu.SemaphoreType.DMA((1 + 2 * nb,)),
            ],
            compiler_params=pltpu.CompilerParams(
                collective_id=0, has_side_effects=True, vmem_limit_bytes=67_000_000
            ),
        )(x.reshape(flat), dy.reshape(flat), w_gate[0], w_up[0], w_down[0])
        return tuple(g[None] for g in grads)

    return jax.shard_map(
        step,
        mesh=mesh,
        in_specs=(P("rep", None, None),) * 2 + (P("pp", None, None),) * 3,
        out_specs=(P(("rep", "pp"), None, None),) * 3,
        check_vma=False,
    )
```

```python
import functools

import jax
import jax.numpy as jnp
from jax import lax
from jax.experimental import pallas as pl
from jax.experimental.pallas import tpu as pltpu
from jax.sharding import PartitionSpec as P

CHUNK = 128
BLOCK = 256
HALF = BLOCK // 2
OFF = 5
AHEAD = 5
STRIP = 32
OUT = 4
EPS = 1e-6
F32, BF16 = jnp.float32, jnp.bfloat16
MESH = pl.DeviceIdType.MESH


def dot(a, b):
    return jnp.dot(a, b, preferred_element_type=F32)


def sigmoid(x):
    return 0.5 * jnp.tanh(0.5 * x) + 0.5


def kernel(
    stages, per, chunks,
    x_ref, dy_ref, wg_ref, wu_ref, wd_ref,
    og_ref, ou_ref, od_ref,
    kept, byin, fout, bout, wgu, wgut, wd, wdt, rhs, lhs, total, mids, slopes,
    fsend, frecv, bsend, brecv, wsem,
):
    me = lax.axis_index("pp")
    behind = stages - 1 - me
    first, last = me == 0, behind == 0
    right, left = lax.rem(me + 1, stages), lax.rem(me + stages - 1, stages)
    d, ff = wg_ref.shape
    nb = ff // HALF
    nd = pl.cdiv(ff, BLOCK)
    quarter = (nb + nd) // per

    loads = [pltpu.make_async_copy(wd_ref, wd, wsem.at[0])]
    for j in range(nb):
        cols = pl.ds(j * HALF, HALF)
        loads.append(pltpu.make_async_copy(wg_ref.at[:, cols], wgu.at[j, :, pl.ds(0, HALF)], wsem.at[1 + 2 * j]))
        loads.append(pltpu.make_async_copy(wu_ref.at[:, cols], wgu.at[j, :, pl.ds(HALF, HALF)], wsem.at[2 + 2 * j]))
    for load in loads:
        load.start()

    reach = OFF * (stages - 1)
    n_kept, n_by, n_mid = kept.shape[0], byin.shape[0], mids.shape[0]
    assert n_kept > reach and n_by > reach and n_mid >= OFF * (stages - 2)

    def x_load(k):
        return pltpu.make_async_copy(x_ref.at[k], kept.at[lax.rem(k, n_kept)], frecv.at[k])

    def dy_load(k):
        return pltpu.make_async_copy(dy_ref.at[k], byin.at[lax.rem(k, n_by)], brecv.at[k])

    @pl.when(first)
    def _():
        def go(k, c):
            x_load(k).start()
            return c

        lax.fori_loop(0, min(chunks, n_kept), go, 0)

    @pl.when(last)
    def _():
        def go(k, c):
            dy_load(k).start()
            return c

        lax.fori_loop(0, min(chunks, n_by), go, 0)

    barrier = pltpu.get_barrier_semaphore()
    for side in (left, right):
        pl.semaphore_signal(barrier, inc=1, device_id={"pp": side}, device_id_type=MESH)

    total[...] = jnp.zeros_like(total)
    rhs[:, nb + nd - 1] = jnp.zeros_like(rhs[:, nb + nd - 1])
    wdt[nd - 1] = jnp.zeros_like(wdt[nd - 1])
    for load in loads:
        load.wait()
    pl.semaphore_wait(barrier, 2)

    def f_copy(k):
        return pltpu.make_async_remote_copy(
            src_ref=fout.at[lax.rem(k, OUT)], dst_ref=kept.at[lax.rem(k, n_kept)], send_sem=fsend.at[k], recv_sem=frecv.at[k],
            device_id={"pp": right}, device_id_type=MESH,
        )

    def b_copy(k):
        return pltpu.make_async_remote_copy(
            src_ref=bout.at[lax.rem(k, OUT)], dst_ref=byin.at[lax.rem(k, n_by)], send_sem=bsend.at[k], recv_sem=brecv.at[k],
            device_id={"pp": left}, device_id_type=MESH,
        )

    def normed(h):
        wide = h.astype(F32)
        scale = lax.rsqrt(jnp.mean(wide * wide, -1, keepdims=True) + EPS)
        return wide, scale, (wide * scale).astype(BF16)

    def forward(k):
        x_load(k).wait()

        @pl.when(k >= OUT)
        def _():
            f_copy(k - OUT).wait_send()

        slot = lax.rem(k, n_mid)
        wide, _, a = normed(kept[lax.rem(k, n_kept)])
        for j in range(nb):
            gu = dot(a, wgu[j])
            g, u = gu[:, :HALF], gu[:, HALF:]
            s = sigmoid(g)
            silu = g * s
            mids[slot, :, j * HALF : (j + 1) * HALF] = (silu * u).astype(BF16)
            slopes[slot, j, :, :HALF] = u * (s + silu * (1.0 - s))
            slopes[slot, j, :, HALF:] = silu
        y = dot(mids[slot], wd[...]).astype(BF16)
        fout[lax.rem(k, OUT)] = (wide + y.astype(F32)).astype(BF16)
        f_copy(k).start()

    def backward(k):
        slot = lax.rem(lax.div(k, per), 2)
        mine = lax.rem(k, n_mid)
        here = lax.rem(k, n_kept)
        rows = pl.ds(pl.multiple_of(lax.rem(k, per) * CHUNK, CHUNK), CHUNK)

        @pl.when(last)
        def _():
            x_load(k).wait()

        @pl.when(jnp.logical_not(first) & (k >= OUT))
        def _():
            b_copy(k - OUT).wait_send()

        dy_load(k).wait()

        def chunk(again, onward):
            by = byin[lax.rem(k, n_by)]
            _, scale, a = normed(kept[here])
            lhs[slot, 0, :, rows] = a.astype(F32).T.astype(BF16)
            lhs[slot, 1, :, rows] = by.astype(F32).T.astype(BF16)
            for jj in range(nd):
                two = dot(by, wdt[jj]).astype(BF16).astype(F32)
                for part in range(min(2, nb - 2 * jj)):
                    j = 2 * jj + part
                    dmid = two[:, part * HALF : (part + 1) * HALF]
                    if again:
                        gu = dot(a, wgu[j])
                        g, u = gu[:, :HALF], gu[:, HALF:]
                        s = sigmoid(g)
                        silu = g * s
                        slope, mid = u * (s + silu * (1.0 - s)), (silu * u).astype(BF16)
                    else:
                        slope, silu = slopes[mine, j, :, :HALF], slopes[mine, j, :, HALF:]
                        mid = mids[mine, :, j * HALF : (j + 1) * HALF]
                    dgate, dup = (dmid * slope).astype(BF16), (dmid * silu).astype(BF16)
                    rhs[slot, nb + jj, rows, part * HALF : (part + 1) * HALF] = mid
                    rhs[slot, j, rows, :HALF] = dgate
                    rhs[slot, j, rows, HALF:] = dup
            if onward:
                da = dot(jnp.concatenate([rhs[slot, j, rows] for j in range(nb)], axis=1), wgut[...])
                for lo in range(0, CHUNK, STRIP):
                    part = slice(lo, lo + STRIP)
                    wide, given = kept[here, part].astype(F32), byin[lax.rem(k, n_by), part].astype(F32)
                    lead, each = scale[part], da[part].astype(BF16).astype(F32)
                    lean = jnp.mean(each * wide, -1, keepdims=True) * lead * lead * lead
                    dh = (each * lead - wide * lean).astype(BF16)
                    bout[lax.rem(k, OUT), part] = (given + dh.astype(F32)).astype(BF16)
                b_copy(k).start()

        @pl.when(first)
        def _():
            chunk(True, False)

        @pl.when(last)
        def _():
            chunk(True, True)

        @pl.when(jnp.logical_not(first | last))
        def _():
            chunk(False, True)

        @pl.when(first & (k + n_kept < chunks))
        def _():
            x_load(k + n_kept).start()

        @pl.when(last & (k + n_by < chunks))
        def _():
            dy_load(k + n_by).start()

    def products(k):
        slot = lax.rem(lax.div(k, per), 2)
        start = lax.rem(k, per) * quarter
        for i in range(quarter):
            q = start + i
            which = jnp.where(q >= nb, 1, 0)
            term = dot(lhs[slot, which], rhs[slot, q]).astype(BF16)
            total[q] += term.astype(F32)

    def transposed():
        for j in range(nb):
            wgut[j * BLOCK : (j + 1) * BLOCK, :] = wgu[j].astype(F32).T.astype(BF16)
        for jj in range(nd):
            lo, hi = jj * BLOCK, min(ff, (jj + 1) * BLOCK)
            wdt[jj, :, : hi - lo] = wd[lo:hi, :].astype(F32).T.astype(BF16)

    def step(i, carry):
        f, b = i, i - OFF * behind
        w = b - per

        @pl.when(i == jnp.where(first, 3, 0))
        def _():
            transposed()

        @pl.when((b >= 0) & (b < chunks))
        def _():
            backward(b)

        @pl.when((f < chunks) & jnp.logical_not(last))
        def _():
            forward(f)

        @pl.when((w >= 0) & (w < chunks))
        def _():
            products(w)

        return carry

    lax.fori_loop(0, chunks + OFF * (stages - 1) + per, step, 0)

    for jj in range(nd):
        lo, hi = jj * BLOCK, min(ff, (jj + 1) * BLOCK)
        od_ref[lo:hi, :] = total[nb + jj].T[: hi - lo].astype(BF16)
    for j in range(nb):
        cols = slice(j * HALF, (j + 1) * HALF)
        og_ref[:, cols] = total[j, :, :HALF].astype(BF16)
        ou_ref[:, cols] = total[j, :, HALF:].astype(BF16)

    def sent(copy):
        def one(k, c):
            copy(k).wait_send()
            return c

        lax.fori_loop(max(0, chunks - OUT), chunks, one, 0)

    @pl.when(jnp.logical_not(last))
    def _():
        sent(f_copy)

    @pl.when(jnp.logical_not(first))
    def _():
        sent(b_copy)


def solution(mesh):
    stages = mesh.shape["pp"]

    def step(x, dy, w_gate, w_up, w_down):
        micro, tokens, d = x.shape
        ff = w_gate.shape[-1]
        per = tokens // CHUNK
        chunks = micro * per
        nb, nd = ff // HALF, pl.cdiv(ff, BLOCK)
        flat = (chunks, CHUNK, d)
        reach, saved = OFF * (stages - 1), OFF * (stages - 2)
        grads = pl.pallas_call(
            functools.partial(kernel, stages, per, chunks),
            out_shape=[
                pltpu.VMEM((d, ff), BF16),
                pltpu.VMEM((d, ff), BF16),
                pltpu.VMEM((ff, d), BF16),
            ],
            in_specs=[pl.BlockSpec(memory_space=pl.ANY)] * 5,
            out_specs=[pl.BlockSpec(memory_space=pltpu.VMEM)] * 3,
            scratch_shapes=[
                pltpu.VMEM((reach + AHEAD, CHUNK, d), BF16),
                pltpu.VMEM((reach + 1, CHUNK, d), BF16),
                pltpu.VMEM((OUT, CHUNK, d), BF16),
                pltpu.VMEM((OUT, CHUNK, d), BF16),
                pltpu.VMEM((nb, d, BLOCK), BF16),
                pltpu.VMEM((nb * BLOCK, d), BF16),
                pltpu.VMEM((ff, d), BF16),
                pltpu.VMEM((nd, d, BLOCK), BF16),
                pltpu.VMEM((2, nb + nd, tokens, BLOCK), BF16),
                pltpu.VMEM((2, 2, d, tokens), BF16),
                pltpu.VMEM((nb + nd, d, BLOCK), F32),
                pltpu.VMEM((saved, CHUNK, ff), BF16),
                pltpu.VMEM((saved, nb, CHUNK, BLOCK), F32),
                pltpu.SemaphoreType.DMA((chunks,)),
                pltpu.SemaphoreType.DMA((chunks,)),
                pltpu.SemaphoreType.DMA((chunks,)),
                pltpu.SemaphoreType.DMA((chunks,)),
                pltpu.SemaphoreType.DMA((1 + 2 * nb,)),
            ],
            compiler_params=pltpu.CompilerParams(
                collective_id=0, has_side_effects=True, vmem_limit_bytes=61500000
            ),
        )(x.reshape(flat), dy.reshape(flat), w_gate[0], w_up[0], w_down[0])
        return tuple(g[None] for g in grads)

    return jax.shard_map(
        step,
        mesh=mesh,
        in_specs=(P("rep", None, None),) * 2 + (P("pp", None, None),) * 3,
        out_specs=(P(("rep", "pp"), None, None),) * 3,
        check_vma=False,
    )
```

```python
import functools

import jax
import jax.numpy as jnp
from jax import lax
from jax.experimental import pallas as pl
from jax.experimental.pallas import tpu as pltpu
from jax.sharding import PartitionSpec as P

CHUNK = 128
BLOCK = 256
HALF = BLOCK // 2
OFF = 5
AHEAD = 5
STRIP = 32
OUT = 4
EPS = 1e-6
F32, BF16 = jnp.float32, jnp.bfloat16
MESH = pl.DeviceIdType.MESH


def dot(a, b):
    return jnp.dot(a, b, preferred_element_type=F32)


def sigmoid(x):
    return 0.5 * jnp.tanh(0.5 * x) + 0.5


def kernel(
    stages, per, chunks,
    x_ref, dy_ref, wg_ref, wu_ref, wd_ref,
    og_ref, ou_ref, od_ref,
    kept, byin, fout, bout, wgu, wgut, wd, wdt, rhs, lhs, total, mids, slopes,
    fsend, frecv, bsend, brecv, wsem,
):
    me = lax.axis_index("pp")
    behind = stages - 1 - me
    first, last = me == 0, behind == 0
    right, left = lax.rem(me + 1, stages), lax.rem(me + stages - 1, stages)
    d, ff = wg_ref.shape
    nb = ff // HALF
    nd = pl.cdiv(ff, BLOCK)
    quarter = (nb + nd) // per

    loads = [pltpu.make_async_copy(wd_ref, wd, wsem.at[0])]
    for j in range(nb):
        cols = pl.ds(j * HALF, HALF)
        loads.append(pltpu.make_async_copy(wg_ref.at[:, cols], wgu.at[j, :, pl.ds(0, HALF)], wsem.at[1 + 2 * j]))
        loads.append(pltpu.make_async_copy(wu_ref.at[:, cols], wgu.at[j, :, pl.ds(HALF, HALF)], wsem.at[2 + 2 * j]))
    for load in loads:
        load.start()

    reach = OFF * (stages - 1)
    n_kept, n_by, n_mid = kept.shape[0], byin.shape[0], mids.shape[0]
    assert n_kept > reach and n_by > reach and n_mid >= OFF * (stages - 2)

    def x_load(k):
        return pltpu.make_async_copy(x_ref.at[k], kept.at[lax.rem(k, n_kept)], frecv.at[k])

    def dy_load(k):
        return pltpu.make_async_copy(dy_ref.at[k], byin.at[lax.rem(k, n_by)], brecv.at[k])

    @pl.when(first)
    def _():
        def go(k, c):
            x_load(k).start()
            return c

        lax.fori_loop(0, min(chunks, n_kept), go, 0)

    @pl.when(last)
    def _():
        def go(k, c):
            dy_load(k).start()
            return c

        lax.fori_loop(0, min(chunks, n_by), go, 0)

    barrier = pltpu.get_barrier_semaphore()
    for side in (left, right):
        pl.semaphore_signal(barrier, inc=1, device_id={"pp": side}, device_id_type=MESH)

    total[...] = jnp.zeros_like(total)
    rhs[:, nb + nd - 1] = jnp.zeros_like(rhs[:, nb + nd - 1])
    wdt[nd - 1] = jnp.zeros_like(wdt[nd - 1])
    for load in loads:
        load.wait()
    pl.semaphore_wait(barrier, 2)

    def f_copy(k):
        return pltpu.make_async_remote_copy(
            src_ref=fout.at[lax.rem(k, OUT)], dst_ref=kept.at[lax.rem(k, n_kept)], send_sem=fsend.at[k], recv_sem=frecv.at[k],
            device_id={"pp": right}, device_id_type=MESH,
        )

    def b_copy(k):
        return pltpu.make_async_remote_copy(
            src_ref=bout.at[lax.rem(k, OUT)], dst_ref=byin.at[lax.rem(k, n_by)], send_sem=bsend.at[k], recv_sem=brecv.at[k],
            device_id={"pp": left}, device_id_type=MESH,
        )

    def normed(h):
        wide = h.astype(F32)
        scale = lax.rsqrt(jnp.mean(wide * wide, -1, keepdims=True) + EPS)
        return wide, scale, (wide * scale).astype(BF16)

    def before_forward(k):
        x_load(k).wait()

        @pl.when(k >= OUT)
        def _():
            f_copy(k - OUT).wait_send()

    def forward(k):
        slot = lax.rem(k, n_mid)
        wide, _, a = normed(kept[lax.rem(k, n_kept)])
        for j in range(nb):
            gu = dot(a, wgu[j])
            g, u = gu[:, :HALF], gu[:, HALF:]
            s = sigmoid(g)
            silu = g * s
            mids[slot, :, j * HALF : (j + 1) * HALF] = (silu * u).astype(BF16)
            slopes[slot, j, :, :HALF] = u * (s + silu * (1.0 - s))
            slopes[slot, j, :, HALF:] = silu
        y = dot(mids[slot], wd[...]).astype(BF16)
        fout[lax.rem(k, OUT)] = (wide + y.astype(F32)).astype(BF16)
        f_copy(k).start()

    def before_backward(k):
        @pl.when(last)
        def _():
            x_load(k).wait()

        @pl.when(jnp.logical_not(first) & (k >= OUT))
        def _():
            b_copy(k - OUT).wait_send()

        dy_load(k).wait()

    def backward(k, again, onward):
        slot = lax.rem(lax.div(k, per), 2)
        mine = lax.rem(k, n_mid)
        here = lax.rem(k, n_kept)
        rows = pl.ds(pl.multiple_of(lax.rem(k, per) * CHUNK, CHUNK), CHUNK)
        by = byin[lax.rem(k, n_by)]
        _, scale, a = normed(kept[here])
        for jj in range(nd):
            two = dot(by, wdt[jj]).astype(BF16).astype(F32)
            for part in range(min(2, nb - 2 * jj)):
                j = 2 * jj + part
                dmid = two[:, part * HALF : (part + 1) * HALF]
                if again:
                    gu = dot(a, wgu[j])
                    g, u = gu[:, :HALF], gu[:, HALF:]
                    s = sigmoid(g)
                    silu = g * s
                    slope, mid = u * (s + silu * (1.0 - s)), (silu * u).astype(BF16)
                else:
                    slope, silu = slopes[mine, j, :, :HALF], slopes[mine, j, :, HALF:]
                    mid = mids[mine, :, j * HALF : (j + 1) * HALF]
                dgate, dup = (dmid * slope).astype(BF16), (dmid * silu).astype(BF16)
                rhs[slot, nb + jj, rows, part * HALF : (part + 1) * HALF] = mid
                rhs[slot, j, rows, :HALF] = dgate
                rhs[slot, j, rows, HALF:] = dup
        if onward:
            da = dot(jnp.concatenate([rhs[slot, j, rows] for j in range(nb)], axis=1), wgut[...])
            for lo in range(0, CHUNK, STRIP):
                part = slice(lo, lo + STRIP)
                wide, given = kept[here, part].astype(F32), byin[lax.rem(k, n_by), part].astype(F32)
                lead, each = scale[part], da[part].astype(BF16).astype(F32)
                lean = jnp.mean(each * wide, -1, keepdims=True) * lead * lead * lead
                dh = (each * lead - wide * lean).astype(BF16)
                bout[lax.rem(k, OUT), part] = (given + dh.astype(F32)).astype(BF16)
            b_copy(k).start()

    def turned(k):
        slot = lax.rem(lax.div(k, per), 2)
        rows = pl.ds(pl.multiple_of(lax.rem(k, per) * CHUNK, CHUNK), CHUNK)
        lhs[slot, 0, :, rows] = normed(kept[lax.rem(k, n_kept)])[2].astype(F32).T.astype(BF16)
        lhs[slot, 1, :, rows] = byin[lax.rem(k, n_by)].astype(F32).T.astype(BF16)

    def after_backward(k):
        @pl.when(first & (k + n_kept < chunks))
        def _():
            x_load(k + n_kept).start()

        @pl.when(last & (k + n_by < chunks))
        def _():
            dy_load(k + n_by).start()

    def products(k):
        slot = lax.rem(lax.div(k, per), 2)
        start = lax.rem(k, per) * quarter
        for i in range(quarter):
            q = start + i
            which = jnp.where(q >= nb, 1, 0)
            term = dot(lhs[slot, which], rhs[slot, q]).astype(BF16)
            total[q] += term.astype(F32)

    def transposed():
        for j in range(nb):
            wgut[j * BLOCK : (j + 1) * BLOCK, :] = wgu[j].astype(F32).T.astype(BF16)
        for jj in range(nd):
            lo, hi = jj * BLOCK, min(ff, (jj + 1) * BLOCK)
            wdt[jj, :, : hi - lo] = wd[lo:hi, :].astype(F32).T.astype(BF16)

    middle = jnp.logical_not(first | last)

    def step(i, carry):
        f, b = i, i - OFF * behind
        w = b - per
        f_on = (f < chunks) & jnp.logical_not(last)
        b_on = (b >= 0) & (b < chunks)

        @pl.when(i == jnp.where(first, 3, 0))
        def _():
            transposed()

        @pl.when(b_on)
        def _():
            before_backward(b)

        @pl.when(b_on & first)
        def _():
            backward(b, True, False)

        @pl.when(b_on & middle)
        def _():
            backward(b, False, True)

        @pl.when(b_on & last)
        def _():
            backward(b, True, True)

        @pl.when(f_on)
        def _():
            before_forward(f)
            forward(f)

        @pl.when(b_on & (w >= 0))
        def _():
            products(w)
            turned(b)

        @pl.when(b_on & (w < 0))
        def _():
            turned(b)

        @pl.when(b_on)
        def _():
            after_backward(b)

        return carry

    lax.fori_loop(0, chunks + OFF * (stages - 1), step, 0)

    slot = (chunks // per - 1) % 2
    for q in list(range(nb, nb + nd)) + list(range(nb)):
        term = dot(lhs[slot, 1 if q >= nb else 0], rhs[slot, q]).astype(BF16)
        done = total[q] + term.astype(F32)
        if q >= nb:
            lo, hi = (q - nb) * BLOCK, min(ff, (q - nb + 1) * BLOCK)
            od_ref[lo:hi, :] = done.T[: hi - lo].astype(BF16)
        else:
            cols = slice(q * HALF, (q + 1) * HALF)
            og_ref[:, cols] = done[:, :HALF].astype(BF16)
            ou_ref[:, cols] = done[:, HALF:].astype(BF16)

    def sent(copy):
        def one(k, c):
            copy(k).wait_send()
            return c

        lax.fori_loop(max(0, chunks - OUT), chunks, one, 0)

    @pl.when(jnp.logical_not(last))
    def _():
        sent(f_copy)

    @pl.when(jnp.logical_not(first))
    def _():
        sent(b_copy)


def put(*refs):
    n = (len(refs) - 1) // 2
    copies = [pltpu.make_async_copy(refs[i], refs[n + i], refs[-1].at[i]) for i in range(n)]
    for copy in copies:
        copy.start()
    for copy in copies:
        copy.wait()


def solution(mesh):
    stages = mesh.shape["pp"]

    def step(x, dy, w_gate, w_up, w_down):
        micro, tokens, d = x.shape
        ff = w_gate.shape[-1]
        per = tokens // CHUNK
        chunks = micro * per
        nb, nd = ff // HALF, pl.cdiv(ff, BLOCK)
        flat = (chunks, CHUNK, d)
        reach, saved = OFF * (stages - 1), OFF * (stages - 2)
        grads = pl.pallas_call(
            functools.partial(kernel, stages, per, chunks),
            out_shape=[
                pltpu.VMEM((d, ff), BF16),
                pltpu.VMEM((d, ff), BF16),
                pltpu.VMEM((ff, d), BF16),
            ],
            in_specs=[pl.BlockSpec(memory_space=pl.ANY)] * 5,
            out_specs=[pl.BlockSpec(memory_space=pltpu.VMEM)] * 3,
            scratch_shapes=[
                pltpu.VMEM((reach + AHEAD, CHUNK, d), BF16),
                pltpu.VMEM((reach + 1, CHUNK, d), BF16),
                pltpu.VMEM((OUT, CHUNK, d), BF16),
                pltpu.VMEM((OUT, CHUNK, d), BF16),
                pltpu.VMEM((nb, d, BLOCK), BF16),
                pltpu.VMEM((nb * BLOCK, d), BF16),
                pltpu.VMEM((ff, d), BF16),
                pltpu.VMEM((nd, d, BLOCK), BF16),
                pltpu.VMEM((2, nb + nd, tokens, BLOCK), BF16),
                pltpu.VMEM((2, 2, d, tokens), BF16),
                pltpu.VMEM((nb + nd, d, BLOCK), F32),
                pltpu.VMEM((saved, CHUNK, ff), BF16),
                pltpu.VMEM((saved, nb, CHUNK, BLOCK), F32),
                pltpu.SemaphoreType.DMA((chunks,)),
                pltpu.SemaphoreType.DMA((chunks,)),
                pltpu.SemaphoreType.DMA((chunks,)),
                pltpu.SemaphoreType.DMA((chunks,)),
                pltpu.SemaphoreType.DMA((1 + 2 * nb,)),
            ],
            compiler_params=pltpu.CompilerParams(
                collective_id=0, has_side_effects=True, vmem_limit_bytes=61500000
            ),
        )(x.reshape(flat), dy.reshape(flat), w_gate[0], w_up[0], w_down[0])
        grads = pl.pallas_call(
            put,
            out_shape=[jax.ShapeDtypeStruct(g.shape, g.dtype) for g in grads],
            in_specs=[pl.BlockSpec(memory_space=pl.ANY)] * 3,
            out_specs=[pl.BlockSpec(memory_space=pl.ANY)] * 3,
            scratch_shapes=[pltpu.SemaphoreType.DMA((3,))],
            compiler_params=pltpu.CompilerParams(vmem_limit_bytes=1_000_000),
        )(*grads)
        return tuple(g[None] for g in grads)

    return jax.shard_map(
        step,
        mesh=mesh,
        in_specs=(P("rep", None, None),) * 2 + (P("pp", None, None),) * 3,
        out_specs=(P(("rep", "pp"), None, None),) * 3,
        check_vma=False,
    )
```

```python
import functools

import jax
import jax.numpy as jnp
from jax import lax
from jax.experimental import pallas as pl
from jax.experimental.pallas import tpu as pltpu
from jax.sharding import PartitionSpec as P

CHUNK = 128
BLOCK = 256
HALF = BLOCK // 2
OFF = 4
MORE = 1
AHEAD = 5
STRIP = 32
OUT = 4
EPS = 1e-6
F32, BF16 = jnp.float32, jnp.bfloat16
MESH = pl.DeviceIdType.MESH


def dot(a, b):
    return jnp.dot(a, b, preferred_element_type=F32)


def sigmoid(x):
    return 0.5 * jnp.tanh(0.5 * x) + 0.5


def kernel(
    stages, per, chunks,
    x_ref, dy_ref, wg_ref, wu_ref, wd_ref,
    og_ref, ou_ref, od_ref,
    kept, byin, fout, bout, wgu, wgut, wd, wdt, rhs, lhs, total, mids, slopes,
    fsend, frecv, bsend, brecv, wsem,
):
    me = lax.axis_index("pp")
    behind = stages - 1 - me
    first, last = me == 0, behind == 0
    right, left = lax.rem(me + 1, stages), lax.rem(me + stages - 1, stages)
    d, ff = wg_ref.shape
    nb = ff // HALF
    nd = pl.cdiv(ff, BLOCK)
    quarter = (nb + nd) // per

    barrier = pltpu.get_barrier_semaphore()
    for side in (left, right):
        pl.semaphore_signal(barrier, inc=1, device_id={"pp": side}, device_id_type=MESH)

    loads = []
    for j in range(nb):
        cols = pl.ds(j * HALF, HALF)
        loads.append(pltpu.make_async_copy(wg_ref.at[:, cols], wgu.at[j, :, pl.ds(0, HALF)], wsem.at[1 + 2 * j]))
        loads.append(pltpu.make_async_copy(wu_ref.at[:, cols], wgu.at[j, :, pl.ds(HALF, HALF)], wsem.at[2 + 2 * j]))
    loads.append(pltpu.make_async_copy(wd_ref, wd, wsem.at[0]))

    reach = OFF * (stages - 1) + MORE
    n_kept, n_by, n_mid = kept.shape[0], byin.shape[0], mids.shape[0]
    assert n_kept > reach + 1 and n_by > reach and n_mid > OFF * (stages - 2)

    def x_load(k):
        return pltpu.make_async_copy(x_ref.at[k], kept.at[lax.rem(k, n_kept)], frecv.at[k])

    def dy_load(k):
        return pltpu.make_async_copy(dy_ref.at[k], byin.at[lax.rem(k, n_by)], brecv.at[k])

    @pl.when(first)
    def _():
        x_load(0).start()

    for load in loads:
        load.start()

    @pl.when(first)
    def _():
        def go(k, c):
            x_load(k).start()
            return c

        lax.fori_loop(1, min(chunks, n_kept), go, 0)

    @pl.when(last)
    def _():
        def go(k, c):
            dy_load(k).start()
            return c

        lax.fori_loop(0, min(chunks, n_by), go, 0)

    total[...] = jnp.zeros_like(total)
    rhs[:, nb + nd - 1] = jnp.zeros_like(rhs[:, nb + nd - 1])
    wdt[nd - 1] = jnp.zeros_like(wdt[nd - 1])
    for load in loads:
        load.wait()
    pl.semaphore_wait(barrier, 2)

    def f_copy(k):
        return pltpu.make_async_remote_copy(
            src_ref=fout.at[lax.rem(k, OUT)], dst_ref=kept.at[lax.rem(k, n_kept)], send_sem=fsend.at[k], recv_sem=frecv.at[k],
            device_id={"pp": right}, device_id_type=MESH,
        )

    def b_copy(k):
        return pltpu.make_async_remote_copy(
            src_ref=bout.at[lax.rem(k, OUT)], dst_ref=byin.at[lax.rem(k, n_by)], send_sem=bsend.at[k], recv_sem=brecv.at[k],
            device_id={"pp": left}, device_id_type=MESH,
        )

    def normed(h):
        wide = h.astype(F32)
        scale = lax.rsqrt(jnp.mean(wide * wide, -1, keepdims=True) + EPS)
        return wide, scale, (wide * scale).astype(BF16)

    def before_forward(k):
        x_load(k).wait()

        @pl.when(k >= OUT)
        def _():
            f_copy(k - OUT).wait_send()

    def forward(k):
        slot = lax.rem(k, n_mid)
        wide, _, a = normed(kept[lax.rem(k, n_kept)])
        for j in range(nb):
            gu = dot(a, wgu[j])
            g, u = gu[:, :HALF], gu[:, HALF:]
            s = sigmoid(g)
            silu = g * s
            mids[slot, :, j * HALF : (j + 1) * HALF] = (silu * u).astype(BF16)
            slopes[slot, j, :, :HALF] = u * (s + silu * (1.0 - s))
            slopes[slot, j, :, HALF:] = silu
        y = dot(mids[slot], wd[...]).astype(BF16)
        fout[lax.rem(k, OUT)] = (wide + y.astype(F32)).astype(BF16)
        f_copy(k).start()

    def before_backward(k):
        @pl.when(last)
        def _():
            x_load(k).wait()

        @pl.when(jnp.logical_not(first) & (k >= OUT))
        def _():
            b_copy(k - OUT).wait_send()

        dy_load(k).wait()

    def backward(k, again, onward):
        slot = lax.rem(lax.div(k, per), 2)
        mine = lax.rem(k, n_mid)
        here = lax.rem(k, n_kept)
        rows = pl.ds(pl.multiple_of(lax.rem(k, per) * CHUNK, CHUNK), CHUNK)
        by = byin[lax.rem(k, n_by)]
        _, scale, a = normed(kept[here])
        for jj in range(nd):
            two = dot(by, wdt[jj]).astype(BF16).astype(F32)
            for part in range(min(2, nb - 2 * jj)):
                j = 2 * jj + part
                dmid = two[:, part * HALF : (part + 1) * HALF]
                if again:
                    gu = dot(a, wgu[j])
                    g, u = gu[:, :HALF], gu[:, HALF:]
                    s = sigmoid(g)
                    silu = g * s
                    slope, mid = u * (s + silu * (1.0 - s)), (silu * u).astype(BF16)
                else:
                    slope, silu = slopes[mine, j, :, :HALF], slopes[mine, j, :, HALF:]
                    mid = mids[mine, :, j * HALF : (j + 1) * HALF]
                dgate, dup = (dmid * slope).astype(BF16), (dmid * silu).astype(BF16)
                rhs[slot, nb + jj, rows, part * HALF : (part + 1) * HALF] = mid
                rhs[slot, j, rows, :HALF] = dgate
                rhs[slot, j, rows, HALF:] = dup
        if onward:
            da = dot(jnp.concatenate([rhs[slot, j, rows] for j in range(nb)], axis=1), wgut[...])
            for lo in range(0, CHUNK, STRIP):
                part = slice(lo, lo + STRIP)
                wide, given = kept[here, part].astype(F32), byin[lax.rem(k, n_by), part].astype(F32)
                lead, each = scale[part], da[part].astype(BF16).astype(F32)
                lean = jnp.mean(each * wide, -1, keepdims=True) * lead * lead * lead
                dh = (each * lead - wide * lean).astype(BF16)
                bout[lax.rem(k, OUT), part] = (given + dh.astype(F32)).astype(BF16)
            b_copy(k).start()

    def turned(k):
        slot = lax.rem(lax.div(k, per), 2)
        rows = pl.ds(pl.multiple_of(lax.rem(k, per) * CHUNK, CHUNK), CHUNK)
        lhs[slot, 0, :, rows] = normed(kept[lax.rem(k, n_kept)])[2].astype(F32).T.astype(BF16)
        lhs[slot, 1, :, rows] = byin[lax.rem(k, n_by)].astype(F32).T.astype(BF16)

    def after_backward(k):
        @pl.when(first & (k + n_kept < chunks))
        def _():
            x_load(k + n_kept).start()

        @pl.when(last & (k + n_by < chunks))
        def _():
            dy_load(k + n_by).start()

    def products(k):
        slot = lax.rem(lax.div(k, per), 2)
        start = lax.rem(k, per) * quarter
        for i in range(quarter):
            q = start + i
            which = jnp.where(q >= nb, 1, 0)
            term = dot(lhs[slot, which], rhs[slot, q]).astype(BF16)
            total[q] += term.astype(F32)

    def transposed():
        for j in range(nb):
            wgut[j * BLOCK : (j + 1) * BLOCK, :] = wgu[j].astype(F32).T.astype(BF16)
        for jj in range(nd):
            lo, hi = jj * BLOCK, min(ff, (jj + 1) * BLOCK)
            wdt[jj, :, : hi - lo] = wd[lo:hi, :].astype(F32).T.astype(BF16)

    middle = jnp.logical_not(first | last)

    def step(i, carry):
        f, b = i, i - OFF * behind - jnp.where(first, MORE, 0)
        w = b - per
        f_on = (f < chunks) & jnp.logical_not(last)
        b_on = (b >= 0) & (b < chunks)

        @pl.when(i == jnp.where(first, 3, 0))
        def _():
            transposed()

        @pl.when(f_on)
        def _():
            before_forward(f)
            forward(f)

        @pl.when(b_on)
        def _():
            before_backward(b)

        @pl.when(b_on & first)
        def _():
            backward(b, True, False)

        @pl.when(b_on & middle)
        def _():
            backward(b, False, True)

        @pl.when(b_on & last)
        def _():
            backward(b, True, True)

        @pl.when(b_on & (w >= 0))
        def _():
            products(w)
            turned(b)

        @pl.when(b_on & (w < 0))
        def _():
            turned(b)

        @pl.when(b_on)
        def _():
            after_backward(b)

        return carry

    lax.fori_loop(0, chunks + reach, step, 0)

    slot = (chunks // per - 1) % 2
    for q in list(range(nb, nb + nd)) + list(range(nb)):
        term = dot(lhs[slot, 1 if q >= nb else 0], rhs[slot, q]).astype(BF16)
        done = total[q] + term.astype(F32)
        if q >= nb:
            lo, hi = (q - nb) * BLOCK, min(ff, (q - nb + 1) * BLOCK)
            od_ref[lo:hi, :] = done.T[: hi - lo].astype(BF16)
        else:
            cols = slice(q * HALF, (q + 1) * HALF)
            og_ref[:, cols] = done[:, :HALF].astype(BF16)
            ou_ref[:, cols] = done[:, HALF:].astype(BF16)

    def sent(copy):
        def one(k, c):
            copy(k).wait_send()
            return c

        lax.fori_loop(max(0, chunks - OUT), chunks, one, 0)

    @pl.when(jnp.logical_not(last))
    def _():
        sent(f_copy)

    @pl.when(jnp.logical_not(first))
    def _():
        sent(b_copy)


def put(*refs):
    n = (len(refs) - 1) // 2
    copies = [pltpu.make_async_copy(refs[i], refs[n + i], refs[-1].at[i]) for i in range(n)]
    for copy in copies:
        copy.start()
    for copy in copies:
        copy.wait()


def solution(mesh):
    stages = mesh.shape["pp"]

    def step(x, dy, w_gate, w_up, w_down):
        micro, tokens, d = x.shape
        ff = w_gate.shape[-1]
        per = tokens // CHUNK
        chunks = micro * per
        nb, nd = ff // HALF, pl.cdiv(ff, BLOCK)
        flat = (chunks, CHUNK, d)
        reach, saved = OFF * (stages - 1) + MORE, OFF * (stages - 2) + 1
        grads = pl.pallas_call(
            functools.partial(kernel, stages, per, chunks),
            out_shape=[
                pltpu.VMEM((d, ff), BF16),
                pltpu.VMEM((d, ff), BF16),
                pltpu.VMEM((ff, d), BF16),
            ],
            in_specs=[pl.BlockSpec(memory_space=pl.ANY)] * 5,
            out_specs=[pl.BlockSpec(memory_space=pltpu.VMEM)] * 3,
            scratch_shapes=[
                pltpu.VMEM((reach + AHEAD, CHUNK, d), BF16),
                pltpu.VMEM((reach + 1, CHUNK, d), BF16),
                pltpu.VMEM((OUT, CHUNK, d), BF16),
                pltpu.VMEM((OUT, CHUNK, d), BF16),
                pltpu.VMEM((nb, d, BLOCK), BF16),
                pltpu.VMEM((nb * BLOCK, d), BF16),
                pltpu.VMEM((ff, d), BF16),
                pltpu.VMEM((nd, d, BLOCK), BF16),
                pltpu.VMEM((2, nb + nd, tokens, BLOCK), BF16),
                pltpu.VMEM((2, 2, d, tokens), BF16),
                pltpu.VMEM((nb + nd, d, BLOCK), F32),
                pltpu.VMEM((saved, CHUNK, ff), BF16),
                pltpu.VMEM((saved, nb, CHUNK, BLOCK), F32),
                pltpu.SemaphoreType.DMA((chunks,)),
                pltpu.SemaphoreType.DMA((chunks,)),
                pltpu.SemaphoreType.DMA((chunks,)),
                pltpu.SemaphoreType.DMA((chunks,)),
                pltpu.SemaphoreType.DMA((1 + 2 * nb,)),
            ],
            compiler_params=pltpu.CompilerParams(
                collective_id=0, has_side_effects=True, vmem_limit_bytes=61500000
            ),
        )(x.reshape(flat), dy.reshape(flat), w_gate[0], w_up[0], w_down[0])
        grads = pl.pallas_call(
            put,
            out_shape=[jax.ShapeDtypeStruct(g.shape, g.dtype) for g in grads],
            in_specs=[pl.BlockSpec(memory_space=pl.ANY)] * 3,
            out_specs=[pl.BlockSpec(memory_space=pl.ANY)] * 3,
            scratch_shapes=[pltpu.SemaphoreType.DMA((3,))],
            compiler_params=pltpu.CompilerParams(vmem_limit_bytes=1_000_000),
        )(*grads)
        return tuple(g[None] for g in grads)

    return jax.shard_map(
        step,
        mesh=mesh,
        in_specs=(P("rep", None, None),) * 2 + (P("pp", None, None),) * 3,
        out_specs=(P(("rep", "pp"), None, None),) * 3,
        check_vma=False,
    )
```

```python
import functools

import jax
import jax.numpy as jnp
from jax import lax
from jax.experimental import pallas as pl
from jax.experimental.pallas import tpu as pltpu
from jax.sharding import PartitionSpec as P

CHUNK = 128
BLOCK = 256
HALF = BLOCK // 2
OFF = 4
MORE = 1
AHEAD = 5
STRIP = 32
SHIP = 4
OUT = 4
EPS = 1e-6
F32, BF16 = jnp.float32, jnp.bfloat16
MESH = pl.DeviceIdType.MESH


def dot(a, b):
    return jnp.dot(a, b, preferred_element_type=F32)


def sigmoid(x):
    return 0.5 * jnp.tanh(0.5 * x) + 0.5


def kernel(
    stages, per, chunks,
    x_ref, dy_ref, wg_ref, wu_ref, wd_ref,
    total, lhs, rhs,
    kept, byin, fout, bout, wgu, wgut, wd, wdt, mids, slopes,
    fsend, frecv, bsend, brecv, wsem,
):
    me = lax.axis_index("pp")
    behind = stages - 1 - me
    first, last = me == 0, behind == 0
    right, left = lax.rem(me + 1, stages), lax.rem(me + stages - 1, stages)
    d, ff = wg_ref.shape
    nb = ff // HALF
    nd = pl.cdiv(ff, BLOCK)
    quarter = (nb + nd) // per

    barrier = pltpu.get_barrier_semaphore()
    for side in (left, right):
        pl.semaphore_signal(barrier, inc=1, device_id={"pp": side}, device_id_type=MESH)

    loads = []
    for j in range(nb):
        cols = pl.ds(j * HALF, HALF)
        loads.append(pltpu.make_async_copy(wg_ref.at[:, cols], wgu.at[j, :, pl.ds(0, HALF)], wsem.at[1 + 2 * j]))
        loads.append(pltpu.make_async_copy(wu_ref.at[:, cols], wgu.at[j, :, pl.ds(HALF, HALF)], wsem.at[2 + 2 * j]))
    loads.append(pltpu.make_async_copy(wd_ref, wd, wsem.at[0]))

    reach = OFF * (stages - 1) + MORE
    n_kept, n_by, n_mid = kept.shape[0], byin.shape[0], mids.shape[0]
    assert n_kept > reach + 1 and n_by > reach and n_mid > OFF * (stages - 2)

    def x_load(k):
        return pltpu.make_async_copy(x_ref.at[k], kept.at[lax.rem(k, n_kept)], frecv.at[k])

    def dy_load(k):
        return pltpu.make_async_copy(dy_ref.at[k], byin.at[lax.rem(k, n_by)], brecv.at[k])

    @pl.when(first)
    def _():
        x_load(0).start()

    for load in loads:
        load.start()

    @pl.when(first)
    def _():
        def go(k, c):
            x_load(k).start()
            return c

        lax.fori_loop(1, min(chunks, n_kept), go, 0)

    @pl.when(last)
    def _():
        def go(k, c):
            dy_load(k).start()
            return c

        lax.fori_loop(0, min(chunks, n_by), go, 0)

    total[...] = jnp.zeros_like(total)
    rhs[:, nb + nd - 1] = jnp.zeros_like(rhs[:, nb + nd - 1])
    wdt[nd - 1] = jnp.zeros_like(wdt[nd - 1])
    for load in loads:
        load.wait()
    pl.semaphore_wait(barrier, 2)

    def f_copy(k):
        return pltpu.make_async_remote_copy(
            src_ref=fout.at[lax.rem(k, OUT)], dst_ref=kept.at[lax.rem(k, n_kept)], send_sem=fsend.at[k], recv_sem=frecv.at[k],
            device_id={"pp": right}, device_id_type=MESH,
        )

    def b_copy(k):
        return pltpu.make_async_remote_copy(
            src_ref=bout.at[lax.rem(k, OUT)], dst_ref=byin.at[lax.rem(k, n_by)], send_sem=bsend.at[k], recv_sem=brecv.at[k],
            device_id={"pp": left}, device_id_type=MESH,
        )

    def normed(h):
        wide = h.astype(F32)
        scale = lax.rsqrt(jnp.mean(wide * wide, -1, keepdims=True) + EPS)
        return wide, scale, (wide * scale).astype(BF16)

    def before_forward(k):
        x_load(k).wait()

        @pl.when(k >= OUT)
        def _():
            f_copy(k - OUT).wait_send()

    def forward(k):
        slot = lax.rem(k, n_mid)
        wide, _, a = normed(kept[lax.rem(k, n_kept)])
        for j in range(nb):
            gu = dot(a, wgu[j])
            g, u = gu[:, :HALF], gu[:, HALF:]
            s = sigmoid(g)
            silu = g * s
            mids[slot, :, j * HALF : (j + 1) * HALF] = (silu * u).astype(BF16)
            slopes[slot, j, :, :HALF] = u * (s + silu * (1.0 - s))
            slopes[slot, j, :, HALF:] = silu
        y = dot(mids[slot], wd[...]).astype(BF16)
        fout[lax.rem(k, OUT)] = (wide + y.astype(F32)).astype(BF16)
        f_copy(k).start()

    def before_backward(k):
        @pl.when(last)
        def _():
            x_load(k).wait()

        @pl.when(jnp.logical_not(first) & (k >= OUT))
        def _():
            b_copy(k - OUT).wait_send()

        dy_load(k).wait()

    def backward(k, again, onward):
        slot = lax.rem(lax.div(k, per), 2)
        mine = lax.rem(k, n_mid)
        here = lax.rem(k, n_kept)
        rows = pl.ds(pl.multiple_of(lax.rem(k, per) * CHUNK, CHUNK), CHUNK)
        by = byin[lax.rem(k, n_by)]
        _, scale, a = normed(kept[here])
        for jj in range(nd):
            two = dot(by, wdt[jj]).astype(BF16).astype(F32)
            for part in range(min(2, nb - 2 * jj)):
                j = 2 * jj + part
                dmid = two[:, part * HALF : (part + 1) * HALF]
                if again:
                    gu = dot(a, wgu[j])
                    g, u = gu[:, :HALF], gu[:, HALF:]
                    s = sigmoid(g)
                    silu = g * s
                    slope, mid = u * (s + silu * (1.0 - s)), (silu * u).astype(BF16)
                else:
                    slope, silu = slopes[mine, j, :, :HALF], slopes[mine, j, :, HALF:]
                    mid = mids[mine, :, j * HALF : (j + 1) * HALF]
                dgate, dup = (dmid * slope).astype(BF16), (dmid * silu).astype(BF16)
                rhs[slot, nb + jj, rows, part * HALF : (part + 1) * HALF] = mid
                rhs[slot, j, rows, :HALF] = dgate
                rhs[slot, j, rows, HALF:] = dup
        if onward:
            da = dot(jnp.concatenate([rhs[slot, j, rows] for j in range(nb)], axis=1), wgut[...])
            for lo in range(0, CHUNK, STRIP):
                part = slice(lo, lo + STRIP)
                wide, given = kept[here, part].astype(F32), byin[lax.rem(k, n_by), part].astype(F32)
                lead, each = scale[part], da[part].astype(BF16).astype(F32)
                lean = jnp.mean(each * wide, -1, keepdims=True) * lead * lead * lead
                dh = (each * lead - wide * lean).astype(BF16)
                bout[lax.rem(k, OUT), part] = (given + dh.astype(F32)).astype(BF16)
            b_copy(k).start()

    def turned(k):
        slot = lax.rem(lax.div(k, per), 2)
        rows = pl.ds(pl.multiple_of(lax.rem(k, per) * CHUNK, CHUNK), CHUNK)
        lhs[slot, 0, :, rows] = normed(kept[lax.rem(k, n_kept)])[2].astype(F32).T.astype(BF16)
        lhs[slot, 1, :, rows] = byin[lax.rem(k, n_by)].astype(F32).T.astype(BF16)

    def after_backward(k):
        @pl.when(first & (k + n_kept < chunks))
        def _():
            x_load(k + n_kept).start()

        @pl.when(last & (k + n_by < chunks))
        def _():
            dy_load(k + n_by).start()

    def products(k):
        slot = lax.rem(lax.div(k, per), 2)
        start = lax.rem(k, per) * quarter
        for i in range(quarter):
            q = start + i
            which = jnp.where(q >= nb, 1, 0)
            term = dot(lhs[slot, which], rhs[slot, q]).astype(BF16)
            total[q] += term.astype(F32)

    def transposed():
        for j in range(nb):
            wgut[j * BLOCK : (j + 1) * BLOCK, :] = wgu[j].astype(F32).T.astype(BF16)
        for jj in range(nd):
            lo, hi = jj * BLOCK, min(ff, (jj + 1) * BLOCK)
            wdt[jj, :, : hi - lo] = wd[lo:hi, :].astype(F32).T.astype(BF16)

    middle = jnp.logical_not(first | last)

    def step(i, carry):
        f, b = i, i - OFF * behind - jnp.where(first, MORE, 0)
        w = b - per
        f_on = (f < chunks) & jnp.logical_not(last)
        b_on = (b >= 0) & (b < chunks)

        @pl.when(i == jnp.where(first, 3, 0))
        def _():
            transposed()

        @pl.when(f_on)
        def _():
            before_forward(f)
            forward(f)

        @pl.when(b_on)
        def _():
            before_backward(b)

        @pl.when(b_on & first)
        def _():
            backward(b, True, False)

        @pl.when(b_on & middle)
        def _():
            backward(b, False, True)

        @pl.when(b_on & last)
        def _():
            backward(b, True, True)

        @pl.when(b_on & (w >= 0))
        def _():
            products(w)
            turned(b)

        @pl.when(b_on & (w < 0))
        def _():
            turned(b)

        @pl.when(b_on)
        def _():
            after_backward(b)

        return carry

    lax.fori_loop(0, chunks + reach, step, 0)

    def sent(copy):
        def one(k, c):
            copy(k).wait_send()
            return c

        lax.fori_loop(max(0, chunks - OUT), chunks, one, 0)

    @pl.when(jnp.logical_not(last))
    def _():
        sent(f_copy)

    @pl.when(jnp.logical_not(first))
    def _():
        sent(b_copy)


def finish(slot, nb, total, lhs, rhs, og_ref, ou_ref, od_ref, og, ou, od, sem):
    ff = od.shape[0]
    nd = total.shape[0] - nb
    copies = []

    def leave(source, target):
        copies.append(pltpu.make_async_copy(source, target, sem.at[len(copies)]))
        copies[-1].start()

    for q in [*range(nb, nb + nd), *range(nb)]:
        term = dot(lhs[slot, 1 if q >= nb else 0], rhs[slot, q]).astype(BF16)
        done = total[q] + term.astype(F32)
        if q >= nb:
            lo, hi = (q - nb) * BLOCK, min(ff, (q - nb + 1) * BLOCK)
            od[lo:hi, :] = done.T[: hi - lo].astype(BF16)
            if q == nb + nd - 1:
                leave(od, od_ref)
        else:
            cols = slice(q * HALF, (q + 1) * HALF)
            og[:, cols] = done[:, :HALF].astype(BF16)
            ou[:, cols] = done[:, HALF:].astype(BF16)
            if q % SHIP == SHIP - 1 or q == nb - 1:
                lo = q // SHIP * SHIP * HALF
                cols = pl.ds(lo, (q + 1) * HALF - lo)
                leave(og.at[:, cols], og_ref.at[:, cols])
                leave(ou.at[:, cols], ou_ref.at[:, cols])
    for copy in copies:
        copy.wait()


def solution(mesh):
    stages = mesh.shape["pp"]

    def step(x, dy, w_gate, w_up, w_down):
        micro, tokens, d = x.shape
        ff = w_gate.shape[-1]
        per = tokens // CHUNK
        chunks = micro * per
        nb, nd = ff // HALF, pl.cdiv(ff, BLOCK)
        flat = (chunks, CHUNK, d)
        reach, saved = OFF * (stages - 1) + MORE, OFF * (stages - 2) + 1
        sums = pl.pallas_call(
            functools.partial(kernel, stages, per, chunks),
            out_shape=[
                pltpu.VMEM((nb + nd, d, BLOCK), F32),
                pltpu.VMEM((2, 2, d, tokens), BF16),
                pltpu.VMEM((2, nb + nd, tokens, BLOCK), BF16),
            ],
            in_specs=[pl.BlockSpec(memory_space=pl.ANY)] * 5,
            out_specs=[pl.BlockSpec(memory_space=pltpu.VMEM)] * 3,
            scratch_shapes=[
                pltpu.VMEM((reach + AHEAD, CHUNK, d), BF16),
                pltpu.VMEM((reach + 1, CHUNK, d), BF16),
                pltpu.VMEM((OUT, CHUNK, d), BF16),
                pltpu.VMEM((OUT, CHUNK, d), BF16),
                pltpu.VMEM((nb, d, BLOCK), BF16),
                pltpu.VMEM((nb * BLOCK, d), BF16),
                pltpu.VMEM((ff, d), BF16),
                pltpu.VMEM((nd, d, BLOCK), BF16),
                pltpu.VMEM((saved, CHUNK, ff), BF16),
                pltpu.VMEM((saved, nb, CHUNK, BLOCK), F32),
                pltpu.SemaphoreType.DMA((chunks,)),
                pltpu.SemaphoreType.DMA((chunks,)),
                pltpu.SemaphoreType.DMA((chunks,)),
                pltpu.SemaphoreType.DMA((chunks,)),
                pltpu.SemaphoreType.DMA((1 + 2 * nb,)),
            ],
            compiler_params=pltpu.CompilerParams(
                collective_id=0, has_side_effects=True, vmem_limit_bytes=43_000_000
            ),
        )(x.reshape(flat), dy.reshape(flat), w_gate[0], w_up[0], w_down[0])
        shapes = [(d, ff), (d, ff), (ff, d)]
        grads = pl.pallas_call(
            functools.partial(finish, (micro - 1) % 2, nb),
            out_shape=[jax.ShapeDtypeStruct(shape, BF16) for shape in shapes],
            in_specs=[pl.BlockSpec(memory_space=pltpu.VMEM)] * 3,
            out_specs=[pl.BlockSpec(memory_space=pl.ANY)] * 3,
            scratch_shapes=[*(pltpu.VMEM(shape, BF16) for shape in shapes), pltpu.SemaphoreType.DMA((2 * nb + 1,))],
            compiler_params=pltpu.CompilerParams(vmem_limit_bytes=16_000_000),
        )(*sums)
        return tuple(g[None] for g in grads)

    return jax.shard_map(
        step,
        mesh=mesh,
        in_specs=(P("rep", None, None),) * 2 + (P("pp", None, None),) * 3,
        out_specs=(P(("rep", "pp"), None, None),) * 3,
        check_vma=False,
    )
```

```python
import functools

import jax
import jax.numpy as jnp
from jax import lax
from jax.experimental import pallas as pl
from jax.experimental.pallas import tpu as pltpu
from jax.sharding import PartitionSpec as P

CHUNK = 128
BLOCK = 256
HALF = BLOCK // 2
OFF = 4
MORE = 1
AHEAD = 5
STRIP = 32
SHIP = 4
OUT = 4
EPS = 1e-6
F32, BF16 = jnp.float32, jnp.bfloat16
MESH = pl.DeviceIdType.MESH


def dot(a, b):
    return jnp.dot(a, b, preferred_element_type=F32)


def sigmoid(x):
    return 0.5 * jnp.tanh(0.5 * x) + 0.5


def kernel(
    stages, per, chunks,
    x_ref, dy_ref, wg_ref, wu_ref, wd_ref,
    total, lhs, rhs,
    kept, byin, fout, bout, wgu, wgut, wd, wdt, mids, slopes,
    fsend, frecv, bsend, brecv, wsem,
):
    me = lax.axis_index("pp")
    behind = stages - 1 - me
    first, last = me == 0, behind == 0
    right, left = lax.rem(me + 1, stages), lax.rem(me + stages - 1, stages)
    d, ff = wg_ref.shape
    nb = ff // HALF
    nd = pl.cdiv(ff, BLOCK)
    quarter = (nb + nd) // per

    barrier = pltpu.get_barrier_semaphore()
    for side in (left, right):
        pl.semaphore_signal(barrier, inc=1, device_id={"pp": side}, device_id_type=MESH)

    loads = []
    for j in range(nb):
        cols = pl.ds(j * HALF, HALF)
        loads.append(pltpu.make_async_copy(wg_ref.at[:, cols], wgu.at[j, :, pl.ds(0, HALF)], wsem.at[1 + 2 * j]))
        loads.append(pltpu.make_async_copy(wu_ref.at[:, cols], wgu.at[j, :, pl.ds(HALF, HALF)], wsem.at[2 + 2 * j]))
    loads.append(pltpu.make_async_copy(wd_ref, wd, wsem.at[0]))

    reach = OFF * (stages - 1) + MORE
    n_kept, n_by, n_mid = kept.shape[0], byin.shape[0], mids.shape[0]
    assert n_kept > reach + 1 and n_by > reach and n_mid > OFF * (stages - 2) and n_mid <= reach

    def x_load(k):
        return pltpu.make_async_copy(x_ref.at[k], kept.at[lax.rem(k, n_kept)], frecv.at[k])

    def dy_load(k):
        return pltpu.make_async_copy(dy_ref.at[k], byin.at[lax.rem(k, n_by)], brecv.at[k])

    @pl.when(first)
    def _():
        x_load(0).start()

    for load in loads:
        load.start()

    @pl.when(first)
    def _():
        def go(k, c):
            x_load(k).start()
            return c

        lax.fori_loop(1, min(chunks, n_kept), go, 0)

    @pl.when(last)
    def _():
        def go(k, c):
            dy_load(k).start()
            return c

        lax.fori_loop(0, min(chunks, n_by), go, 0)

    total[...] = jnp.zeros_like(total)
    rhs[:, nb + nd - 1] = jnp.zeros_like(rhs[:, nb + nd - 1])
    wdt[nd - 1] = jnp.zeros_like(wdt[nd - 1])
    for load in loads:
        load.wait()
    pl.semaphore_wait(barrier, 2)

    def f_copy(k):
        return pltpu.make_async_remote_copy(
            src_ref=fout.at[lax.rem(k, OUT)], dst_ref=kept.at[lax.rem(k, n_kept)], send_sem=fsend.at[k], recv_sem=frecv.at[k],
            device_id={"pp": right}, device_id_type=MESH,
        )

    def b_copy(k):
        return pltpu.make_async_remote_copy(
            src_ref=bout.at[lax.rem(k, OUT)], dst_ref=byin.at[lax.rem(k, n_by)], send_sem=bsend.at[k], recv_sem=brecv.at[k],
            device_id={"pp": left}, device_id_type=MESH,
        )

    def normed(h):
        wide = h.astype(F32)
        scale = lax.rsqrt(jnp.mean(wide * wide, -1, keepdims=True) + EPS)
        return wide, scale, (wide * scale).astype(BF16)

    def before_forward(k):
        x_load(k).wait()

        @pl.when(k >= OUT)
        def _():
            f_copy(k - OUT).wait_send()

    def forward(k):
        slot = lax.rem(k, n_mid)
        wide, _, a = normed(kept[lax.rem(k, n_kept)])
        for j in range(nb):
            gu = dot(a, wgu[j])
            g, u = gu[:, :HALF], gu[:, HALF:]
            s = sigmoid(g)
            silu = g * s
            mids[slot, :, j * HALF : (j + 1) * HALF] = (silu * u).astype(BF16)
            slopes[slot, j, :, :HALF] = u * (s + silu * (1.0 - s))
            slopes[slot, j, :, HALF:] = silu
        y = dot(mids[slot], wd[...]).astype(BF16)
        fout[lax.rem(k, OUT)] = (wide + y.astype(F32)).astype(BF16)
        f_copy(k).start()

    def before_backward(k):
        @pl.when(last)
        def _():
            x_load(k).wait()

        @pl.when(jnp.logical_not(first) & (k >= OUT))
        def _():
            b_copy(k - OUT).wait_send()

        dy_load(k).wait()

    def backward(k, again, onward):
        slot = lax.rem(lax.div(k, per), 2)
        mine = lax.rem(k, n_mid)
        here = lax.rem(k, n_kept)
        rows = pl.ds(pl.multiple_of(lax.rem(k, per) * CHUNK, CHUNK), CHUNK)
        by = byin[lax.rem(k, n_by)]
        _, scale, a = normed(kept[here])
        for jj in range(nd):
            two = dot(by, wdt[jj]).astype(BF16).astype(F32)
            for part in range(min(2, nb - 2 * jj)):
                j = 2 * jj + part
                dmid = two[:, part * HALF : (part + 1) * HALF]
                if again:
                    gu = dot(a, wgu[j])
                    g, u = gu[:, :HALF], gu[:, HALF:]
                    s = sigmoid(g)
                    silu = g * s
                    slope, mid = u * (s + silu * (1.0 - s)), (silu * u).astype(BF16)
                else:
                    slope, silu = slopes[mine, j, :, :HALF], slopes[mine, j, :, HALF:]
                    mid = mids[mine, :, j * HALF : (j + 1) * HALF]
                dgate, dup = (dmid * slope).astype(BF16), (dmid * silu).astype(BF16)
                rhs[slot, nb + jj, rows, part * HALF : (part + 1) * HALF] = mid
                rhs[slot, j, rows, :HALF] = dgate
                rhs[slot, j, rows, HALF:] = dup
        if onward:
            da = dot(jnp.concatenate([rhs[slot, j, rows] for j in range(nb)], axis=1), wgut[...])
            for lo in range(0, CHUNK, STRIP):
                part = slice(lo, lo + STRIP)
                wide, given = kept[here, part].astype(F32), byin[lax.rem(k, n_by), part].astype(F32)
                lead, each = scale[part], da[part].astype(BF16).astype(F32)
                lean = jnp.mean(each * wide, -1, keepdims=True) * lead * lead * lead
                dh = (each * lead - wide * lean).astype(BF16)
                bout[lax.rem(k, OUT), part] = (given + dh.astype(F32)).astype(BF16)
            b_copy(k).start()

    def turned(k):
        slot = lax.rem(lax.div(k, per), 2)
        rows = pl.ds(pl.multiple_of(lax.rem(k, per) * CHUNK, CHUNK), CHUNK)
        lhs[slot, 0, :, rows] = normed(kept[lax.rem(k, n_kept)])[2].astype(F32).T.astype(BF16)
        lhs[slot, 1, :, rows] = byin[lax.rem(k, n_by)].astype(F32).T.astype(BF16)

    def after_backward(k):
        @pl.when(first & (k + n_kept < chunks))
        def _():
            x_load(k + n_kept).start()

        @pl.when(last & (k + n_by < chunks))
        def _():
            dy_load(k + n_by).start()

    def products(k):
        slot = lax.rem(lax.div(k, per), 2)
        start = lax.rem(k, per) * quarter
        for i in range(quarter):
            q = start + i
            which = jnp.where(q >= nb, 1, 0)
            term = dot(lhs[slot, which], rhs[slot, q]).astype(BF16)
            total[q] += term.astype(F32)

    def transposed():
        for j in range(nb):
            wgut[j * BLOCK : (j + 1) * BLOCK, :] = wgu[j].astype(F32).T.astype(BF16)
        for jj in range(nd):
            lo, hi = jj * BLOCK, min(ff, (jj + 1) * BLOCK)
            wdt[jj, :, : hi - lo] = wd[lo:hi, :].astype(F32).T.astype(BF16)

    middle = jnp.logical_not(first | last)

    def step(i, carry):
        f, b = i, i - OFF * behind - jnp.where(first, MORE, 0)
        w = b - per
        f_on = (f < chunks) & jnp.logical_not(last)
        b_on = (b >= 0) & (b < chunks)

        @pl.when(i == jnp.where(first, 3, 0))
        def _():
            transposed()

        @pl.when(f_on)
        def _():
            before_forward(f)
            forward(f)

        ending = b >= chunks - per

        @pl.when(b_on & ending)
        def _():
            products(w)

        @pl.when(b_on)
        def _():
            before_backward(b)

        held = b >= chunks - n_mid

        @pl.when(b_on & first & jnp.logical_not(held))
        def _():
            backward(b, True, False)

        @pl.when(b_on & first & held)
        def _():
            backward(b, False, False)

        @pl.when(b_on & middle)
        def _():
            backward(b, False, True)

        @pl.when(b_on & last)
        def _():
            backward(b, True, True)

        @pl.when(b_on & (w >= 0) & jnp.logical_not(ending))
        def _():
            products(w)
            turned(b)

        @pl.when(b_on & ((w < 0) | ending))
        def _():
            turned(b)

        @pl.when(b_on)
        def _():
            after_backward(b)

        return carry

    lax.fori_loop(0, chunks + reach, step, 0)

    def sent(copy):
        def one(k, c):
            copy(k).wait_send()
            return c

        lax.fori_loop(max(0, chunks - OUT), chunks, one, 0)

    @pl.when(jnp.logical_not(last))
    def _():
        sent(f_copy)

    @pl.when(jnp.logical_not(first))
    def _():
        sent(b_copy)


def finish(slot, nb, total, lhs, rhs, og_ref, ou_ref, od_ref, og, ou, od, sem):
    ff = od.shape[0]
    nd = total.shape[0] - nb
    copies = []

    def leave(source, target):
        copies.append(pltpu.make_async_copy(source, target, sem.at[len(copies)]))
        copies[-1].start()

    for q in [*range(nb, nb + nd), *range(nb)]:
        term = dot(lhs[slot, 1 if q >= nb else 0], rhs[slot, q]).astype(BF16)
        done = total[q] + term.astype(F32)
        if q >= nb:
            lo, hi = (q - nb) * BLOCK, min(ff, (q - nb + 1) * BLOCK)
            od[lo:hi, :] = done.T[: hi - lo].astype(BF16)
            if q == nb + nd - 1:
                leave(od, od_ref)
        else:
            cols = slice(q * HALF, (q + 1) * HALF)
            og[:, cols] = done[:, :HALF].astype(BF16)
            ou[:, cols] = done[:, HALF:].astype(BF16)
            if q % SHIP == SHIP - 1 or q == nb - 1:
                lo = q // SHIP * SHIP * HALF
                cols = pl.ds(lo, (q + 1) * HALF - lo)
                leave(og.at[:, cols], og_ref.at[:, cols])
                leave(ou.at[:, cols], ou_ref.at[:, cols])
    for copy in copies:
        copy.wait()


def solution(mesh):
    stages = mesh.shape["pp"]

    def step(x, dy, w_gate, w_up, w_down):
        micro, tokens, d = x.shape
        ff = w_gate.shape[-1]
        per = tokens // CHUNK
        chunks = micro * per
        nb, nd = ff // HALF, pl.cdiv(ff, BLOCK)
        flat = (chunks, CHUNK, d)
        reach, saved = OFF * (stages - 1) + MORE, OFF * (stages - 2) + 1
        sums = pl.pallas_call(
            functools.partial(kernel, stages, per, chunks),
            out_shape=[
                pltpu.VMEM((nb + nd, d, BLOCK), F32),
                pltpu.VMEM((2, 2, d, tokens), BF16),
                pltpu.VMEM((2, nb + nd, tokens, BLOCK), BF16),
            ],
            in_specs=[pl.BlockSpec(memory_space=pl.ANY)] * 5,
            out_specs=[pl.BlockSpec(memory_space=pltpu.VMEM)] * 3,
            scratch_shapes=[
                pltpu.VMEM((reach + AHEAD, CHUNK, d), BF16),
                pltpu.VMEM((reach + 1, CHUNK, d), BF16),
                pltpu.VMEM((OUT, CHUNK, d), BF16),
                pltpu.VMEM((OUT, CHUNK, d), BF16),
                pltpu.VMEM((nb, d, BLOCK), BF16),
                pltpu.VMEM((nb * BLOCK, d), BF16),
                pltpu.VMEM((ff, d), BF16),
                pltpu.VMEM((nd, d, BLOCK), BF16),
                pltpu.VMEM((saved, CHUNK, ff), BF16),
                pltpu.VMEM((saved, nb, CHUNK, BLOCK), F32),
                pltpu.SemaphoreType.DMA((chunks,)),
                pltpu.SemaphoreType.DMA((chunks,)),
                pltpu.SemaphoreType.DMA((chunks,)),
                pltpu.SemaphoreType.DMA((chunks,)),
                pltpu.SemaphoreType.DMA((1 + 2 * nb,)),
            ],
            compiler_params=pltpu.CompilerParams(
                collective_id=0, has_side_effects=True, vmem_limit_bytes=43_000_000
            ),
        )(x.reshape(flat), dy.reshape(flat), w_gate[0], w_up[0], w_down[0])
        shapes = [(d, ff), (d, ff), (ff, d)]
        grads = pl.pallas_call(
            functools.partial(finish, (micro - 1) % 2, nb),
            out_shape=[jax.ShapeDtypeStruct(shape, BF16) for shape in shapes],
            in_specs=[pl.BlockSpec(memory_space=pltpu.VMEM)] * 3,
            out_specs=[pl.BlockSpec(memory_space=pl.ANY)] * 3,
            scratch_shapes=[*(pltpu.VMEM(shape, BF16) for shape in shapes), pltpu.SemaphoreType.DMA((2 * nb + 1,))],
            compiler_params=pltpu.CompilerParams(vmem_limit_bytes=16_000_000),
        )(*sums)
        return tuple(g[None] for g in grads)

    return jax.shard_map(
        step,
        mesh=mesh,
        in_specs=(P("rep", None, None),) * 2 + (P("pp", None, None),) * 3,
        out_specs=(P(("rep", "pp"), None, None),) * 3,
        check_vma=False,
    )
```
